256 devices in a mesh: dp: 8 (over z_hi, y), expert: 32 (over z_lo, x, core).
Axes of the slice: x: 4, y: 4, z: 8 (z_hi: 2, z_lo: 4; z = z_hi * 4 + z_lo), core: 2. Of those that a mesh axis runs over, the one named last changes fastest.
Arguments:
- routed: bfloat16 [32768, 7168], P(('dp', 'expert')), may hold values from -160 to 160
- expert_ids: int32 [32768, 8], P(('dp', 'expert')), may hold values from 0 to 255, all different within a row
- norm_gain: bfloat16 [7168], replicated, may hold values from 0.099609375 to 1.8984375
- gate_weight: bfloat16 [32, 7168, 2048], P('expert', None, 'dp'), may hold values from -0.0625 to 0.0625
- up_weight: bfloat16 [32, 7168, 2048], P('expert', None, 'dp'), may hold values from -0.0625 to 0.0625
- down_weight: bfloat16 [32, 2048, 7168], P('expert', 'dp'), may hold values from -0.125 to 0.125
- old_place: int32 [32], replicated, may hold values from 0 to 255, as said below
- new_place: int32 [32], replicated, may hold values from 0 to 255, as said below
- probe_ids: int32 [10240], P(('dp', 'expert')), may hold values from 0 to 127
Outputs:
- expert_load: float32 [256], P('expert')
- expert_energy: float32 [256], P('expert')
- probe_out: bfloat16 [10240, 7168], P(('dp', 'expert'))
The draws below stay inside these ranges and needn't reach their ends.
Inputs may be any that keep to these rules, and one draw needn't show every extreme that they name: `old_place`: 32 different experts. `new_place`: the same 32 experts as old_place, in some order.
All inputs are finite; a program needn't handle non-finite values.
Results may differ from the reference program's by a relative error of at most 0.012.
Values may be sent and summed in bfloat16 or wider, within the bound.
A program may use at most 128 MiB of HBM per device.

```python
import jax
import jax.numpy as jnp
from jax import lax

D = 7168
FF = 2048
TOP = 8
TOK_DEV = 128
PROBE = 40
EXPERTS = 256
SLOTS = 32
TOKENS = 32768
PROBES = 10240
N_DP = 8


def draw_routed(key, part):
    first = jax.random.fold_in(key, 101)
    second = jax.random.fold_in(key, 202)
    third = jax.random.fold_in(key, 303)
    row_scale = jnp.exp(jax.random.uniform(second, (TOKENS, 1), minval=-1.15, maxval=1.15))
    column_scale = jnp.exp(jax.random.uniform(third, (1, D), minval=-1.15, maxval=1.15))
    rising = jnp.exp(jnp.log(3.0) * (jnp.arange(TOKENS, dtype=jnp.float32) / TOKENS - 0.5))[:, None]
    values = jnp.clip(jax.random.normal(first, (TOKENS, D)), -4.0, 4.0)
    return (values * row_scale * column_scale * rising).astype(jnp.bfloat16)


def draw_plan(key):
    base = jax.random.fold_in(key, 17)
    chosen = jax.random.permutation(jax.random.fold_in(base, 1), EXPERTS)[:SLOTS]
    order = jax.random.permutation(jax.random.fold_in(base, 2), SLOTS)
    return (chosen.astype(jnp.int32), jnp.take(chosen, order).astype(jnp.int32))


def draw_old_place(key, part):
    return draw_plan(key)[0]


def draw_new_place(key, part):
    return draw_plan(key)[1]


def with_ends(values, own_key, least, high):
    longest = values.shape.index(max(values.shape))
    spots = []
    for shift in (0, 1):
        where = [jax.random.randint(jax.random.fold_in(own_key, axis), (), 0, length) for axis, length in enumerate(values.shape)]
        where[longest] = (where[longest] + shift) % values.shape[longest]
        spots.append(tuple(where))
    return values.at[spots[0]].set(least).at[spots[1]].set(high)


def block_levels(stream_key, extent, pieces, low, top_value):
    level, own = 1.0, jax.random.fold_in(stream_key, 6)
    for dim, parts in pieces:
        steps = jnp.exp(jax.random.uniform(jax.random.fold_in(own, dim), (parts,), jnp.float32, low / len(pieces), top_value / len(pieces)))
        level = level * jnp.repeat(steps, extent[dim] // parts).reshape([-1 if axis == dim else 1 for axis in range(len(extent))])
    return level


def picks_of(rng, rows, count, top, lift):
    ranking = jax.random.permutation(jax.random.fold_in(rng, 1), count)
    pull = ranking
    for power in range(3):
        pull = pull * pull // count
    pull = pull * lift // count
    tickets = jax.random.randint(jax.random.fold_in(rng, 2), (rows, count), 0, 4096) + pull
    holders = jax.random.permutation(jax.random.fold_in(rng, 3), rows)[jnp.arange(count) % rows]
    tickets = jnp.where(jnp.arange(rows)[:, None] == holders[None, :], 1 << 14, tickets)
    merit = tickets * count + jnp.arange(count)
    return lax.top_k(merit.astype(jnp.int32), top)[1].astype(jnp.int32)


def noise(stream_key, shape, deviation, most, cuts=(), kind=jnp.bfloat16):
    array = deviation * jax.random.normal(stream_key, shape, jnp.float32)
    if cuts:
        array = array * block_levels(stream_key, shape, cuts, -0.22, 0.18)
    return jnp.clip(array, -most, most).astype(kind)


def setup_inputs(seed: int = 0) -> dict:
    seeds = jax.random.split(jax.random.key(seed), 10)
    return {
        "routed": draw_routed(jax.random.fold_in(seeds[9], 71), 0),
        "expert_ids": picks_of(seeds[1], TOKENS, EXPERTS, TOP, 512),
        "norm_gain": jnp.clip(1.0 + 0.18 * jax.random.normal(seeds[2], (D,), jnp.float32), 0.099609375, 1.8984375).astype(jnp.bfloat16),
        "gate_weight": noise(seeds[3], (SLOTS, D, FF), D ** -0.5, 0.0625, ((0, 32), (2, 8))),
        "up_weight": noise(seeds[4], (SLOTS, D, FF), D ** -0.5, 0.0625, ((0, 32), (2, 8))),
        "down_weight": noise(seeds[5], (SLOTS, FF, D), FF ** -0.5, 0.125, ((0, 32), (1, 8))),
        "old_place": draw_old_place(jax.random.fold_in(seeds[9], 71), 0),
        "new_place": draw_new_place(jax.random.fold_in(seeds[9], 71), 0),
        "probe_ids": with_ends(jax.random.randint(seeds[8], (PROBES,), 0, TOK_DEV), jax.random.fold_in(seeds[8], 1), 0, TOK_DEV - 1).astype(jnp.int32),
    }


epsilon = 1e-06

def block_stats(block):
    token_rows, id_block = block
    features = token_rows.astype(jnp.float32)
    mean_square = lax.optimization_barrier(jnp.sum(features * features, axis=1)) / D
    positions = jnp.arange(EXPERTS, dtype=jnp.int32)
    onehot = lax.optimization_barrier(jnp.sum((id_block[:, :, None] == positions[None, None, :]).astype(jnp.float32), axis=1))
    columns = jnp.stack([jnp.ones_like(mean_square), mean_square])
    return (jnp.dot(columns, onehot, precision=lax.Precision.HIGHEST), mean_square)

def reference(routed, expert_ids, norm_gain, gate_weight, up_weight, down_weight, old_place, new_place, probe_ids):
    blocks = TOKENS // TOK_DEV
    stats, mean_square = lax.map(block_stats, (routed.reshape(blocks, TOK_DEV, D), expert_ids.reshape(blocks, TOK_DEV, TOP)))
    totals = lax.optimization_barrier(jnp.sum(stats, axis=0))
    counts = totals[0]
    expert_load = counts * EXPERTS / (TOKENS * TOP)
    expert_energy = totals[1] / counts
    mean_square = mean_square.reshape(TOKENS)
    offsets = jnp.arange(PROBES, dtype=jnp.int32) // PROBE * TOK_DEV
    picked = (offsets + probe_ids).astype(jnp.int32)
    picked_rows = jnp.take(routed, picked, axis=0).astype(jnp.float32)
    scale = lax.rsqrt(jnp.take(mean_square, picked) + epsilon)
    normed = (picked_rows * scale[:, None] * norm_gain.astype(jnp.float32)[None, :]).astype(jnp.bfloat16)
    grouped = normed.reshape(N_DP, SLOTS, PROBE, D)
    slot_index = jnp.arange(SLOTS, dtype=jnp.int32)
    hidden_block = FF // N_DP

    def per_slot(slot_number):
        holder = jnp.sum(jnp.where(old_place == new_place[slot_number], slot_index, 0)).astype(jnp.int32)
        inputs = lax.dynamic_index_in_dim(grouped, slot_number, 1, keepdims=False).reshape(N_DP * PROBE, D)
        gate_matrix = lax.dynamic_index_in_dim(gate_weight, holder, 0, keepdims=False)
        up_matrix = lax.dynamic_index_in_dim(up_weight, holder, 0, keepdims=False)
        down_matrix = lax.dynamic_index_in_dim(down_weight, holder, 0, keepdims=False)
        gate_value = jnp.dot(inputs, gate_matrix, preferred_element_type=jnp.float32)
        up_value = jnp.dot(inputs, up_matrix, preferred_element_type=jnp.float32)
        hidden = (jax.nn.silu(gate_value) * up_value).astype(jnp.bfloat16)
        running = jnp.zeros((N_DP * PROBE, D), jnp.float32)
        for group_index in range(N_DP):
            lower = group_index * hidden_block
            partial_value = jnp.dot(hidden[:, lower:lower + hidden_block], down_matrix[lower:lower + hidden_block], preferred_element_type=jnp.float32).astype(jnp.bfloat16)
            partial_value = lax.optimization_barrier(partial_value)
            running = running + partial_value.astype(jnp.float32)
        return running.astype(jnp.bfloat16).reshape(N_DP, PROBE, D)
    results = lax.map(per_slot, slot_index)
    probe_out = jnp.transpose(results, (1, 0, 2, 3)).reshape(PROBES, D)
    return (expert_load, expert_energy, probe_out)
```

```python
import functools

import jax
import jax.numpy as jnp
from jax import lax
from jax.experimental import pallas as pl
from jax.experimental.pallas import tpu as pltpu
from jax.sharding import PartitionSpec as P

MESH = pl.DeviceIdType.MESH
F32 = jnp.float32
BF16 = jnp.bfloat16
EXP_DEV = 8
TOP = 8
EPS = 1e-06
PC = 256


class Layout:
    def __init__(self, zh=2, y=4, zl=4, x=4, c=2, pieces=7, rows=40, toks=128, hid=256):
        self.ZH, self.Y, self.ZL, self.X, self.C = zh, y, zl, x, c
        self.KP, self.ROWS, self.TOKS, self.HID = pieces, rows, toks, hid
        self.NZ, self.NXC = zh * zl, x * c
        self.NS = zl * x * c
        self.CW = pieces * PC
        self.D = zl * self.CW


def kernel(
    L, tokens,
    tgt_ref, src_ref, pid_ref, ids_ref, gain_ref, routed_hbm, gate_hbm, up_hbm, down_hbm,
    load_ref, energy_ref, out_hbm,
    routed_v, gain_v, gate_v, up_v, down_v,
    send1, recv1, send2, xbuf, gacc, uacc, hid,
    pbuf, ra, rb, bs, sz, zr, f1, fin,
    st_y, st_z, st_x, st_c,
    in_sem, w_sem, s1_send, s1_recv, s2_send, s2_recv, y_send, yp_recv, ym_recv, yf_recv,
    r_send, ra_recv, rb0_recv, rb1_recv, z_send, zr_recv, f_send, f_recv, st_send, st_recv,
):
    Y, ZL, X, C, KP, NZ, NXC, NS, CW = L.Y, L.ZL, L.X, L.C, L.KP, L.NZ, L.NXC, L.NS, L.CW
    rows = L.ROWS
    me_d, me_e = lax.axis_index("dp"), lax.axis_index("expert")
    zh, y = me_d // Y, me_d % Y
    zl, xc = me_e // NXC, me_e % NXC
    x, c = xc // C, xc % C
    p = zh * ZL + zl
    kme = (xc - C * zl + C * NXC) % NXC
    active = kme < KP
    mine = p * NXC + xc

    def dev(z, yy, xcc):
        return ((z // ZL) * Y + yy, (z % ZL) * NXC + xcc)

    def half(r, z_low):
        return ((r - z_low + ZL // 2 - 1 + r % 2 + NZ) % NZ) // ZL

    def cols(k):
        return pl.ds(pl.multiple_of(k * PC, PC), PC)

    def remote(src, dst, send, recv, where):
        pltpu.make_async_remote_copy(
            src_ref=src, dst_ref=dst, send_sem=send, recv_sem=recv, device_id=where, device_id_type=MESH
        ).start()

    def wait(ref, sem):
        pltpu.make_async_copy(ref, ref, sem).wait()

    copy_in = pltpu.make_async_copy(routed_hbm, routed_v, in_sem)
    copy_in.start()
    barrier = pltpu.get_barrier_semaphore()

    @pl.loop(0, NZ * NXC)
    def _(q):
        @pl.when(q != mine)
        def _():
            pl.semaphore_signal(barrier, inc=1, device_id=dev(q // NXC, y, q % NXC), device_id_type=MESH)

    for dy in range(1, Y):
        pl.semaphore_signal(barrier, inc=1, device_id=dev(p, (y + dy) % Y, xc), device_id_type=MESH)

    gain_v[...] = gain_ref[...].astype(F32)
    lane = lax.broadcasted_iota(jnp.int32, (8, L.TOKS), 1)
    sub = lax.broadcasted_iota(jnp.int32, (8, L.TOKS), 0)
    picks = []
    for b in range(rows // 8):
        want = jnp.zeros((8, L.TOKS), jnp.int32)
        for i in range(8):
            want = jnp.where(sub == i, pid_ref[b * 8 + i], want)
        picks.append((lane == want).astype(F32))
    select = jnp.concatenate(picks, axis=0).astype(BF16)

    copy_in.wait()
    for hbm, v in ((gate_hbm, gate_v), (up_hbm, up_v)):
        for m in range(ZL):
            pltpu.make_async_copy(hbm.at[pl.ds(m * CW, CW), :], v.at[m], w_sem).start()
    for m in range(ZL):
        pltpu.make_async_copy(down_hbm.at[:, pl.ds(m * CW, CW)], down_v.at[m], w_sem).start()

    square = jnp.zeros((rows, 1), F32)
    for m in range(ZL):
        picked = jnp.dot(select, routed_v[:, m * CW : (m + 1) * CW], preferred_element_type=F32)
        square += jnp.sum(picked * picked, axis=1, keepdims=True)
        send1[m] = picked.astype(BF16)
    scale = lax.rsqrt(square / L.D + EPS)
    for m in range(ZL):
        for t in range(CW // 128):
            tile = m * (CW // 128) + t
            v = send1[m, :, t * 128 : (t + 1) * 128].astype(F32)
            send1[m, :, t * 128 : (t + 1) * 128] = (v * scale * gain_v[tile : tile + 1, :]).astype(BF16)

    pl.semaphore_wait(barrier, NZ * NXC - 1 + Y - 1)

    @pl.loop(0, ZL * KP)
    def _(i):
        idx = (i + (xc % KP) * ZL + zl) % (ZL * KP)
        m, k = idx % ZL, idx // ZL
        r = m + ZL * ((half(m, zl) + zh) % 2)
        xct = (k + C * m) % NXC

        @pl.when(r * NXC + xct != mine)
        def _():
            remote(send1.at[m, :, cols(k)], recv1.at[me_e], s1_send, s1_recv, dev(r, y, xct))

    def squares(i, acc):
        v = routed_v[:, pl.ds(pl.multiple_of(i * PC, PC), PC)].astype(F32)
        return acc + v * v

    total = lax.fori_loop(0, L.D // PC, squares, jnp.zeros((L.TOKS, PC), F32))
    mean_square = jnp.sum(total, axis=1, keepdims=True) / L.D
    ids = ids_ref[...].astype(F32).T
    expert = lax.broadcasted_iota(jnp.int32, (L.TOKS, 256), 1).astype(F32)
    onehot = jnp.zeros((L.TOKS, 256), F32)
    for k in range(TOP):
        onehot += (ids[:, k : k + 1] == expert).astype(F32)
    counts = jnp.sum(onehot, axis=0, keepdims=True)
    energy = jnp.sum(onehot * mean_square, axis=0, keepdims=True)
    stats = jnp.concatenate(
        [counts[:, :128], counts[:, 128:], energy[:, :128], energy[:, 128:], jnp.zeros((4, 128), F32)], axis=0
    )
    rounds = (
        (st_y, Y, y, lambda o: dev(p, o, xc)),
        (st_z, NZ, p, lambda o: dev(o, y, xc)),
        (st_x, X, x, lambda o: dev(p, y, o * C + c)),
        (st_c, C, c, lambda o: dev(p, y, x * C + o)),
    )

    def stats_store(n, value):
        buf, _, own, _ = rounds[n]
        buf[own] = value

    def stats_send(n):
        buf, size, own, where = rounds[n]
        for step in range(1, size):
            remote(buf.at[own], buf.at[own], st_send.at[n], st_recv.at[n], where((own + step) % size))

    def stats_sum(n):
        buf, size, own, _ = rounds[n]
        if size > 1:
            wait(buf.at[pl.ds(0, size - 1)], st_recv.at[n])
            wait(buf.at[pl.ds(0, size - 1)], st_send.at[n])
        value = buf[0]
        for o in range(1, size):
            value += buf[o]
        return value

    def stats_out(value):
        ratio = value[2:4, :] / value[0:2, :]
        load = value[0:2, :] * (EXP_DEV * NS / (tokens * TOP))
        where = lax.broadcasted_iota(jnp.int32, (2, 128), 0) * 128 + lax.broadcasted_iota(jnp.int32, (2, 128), 1)
        for i in range(EXP_DEV):
            hit = where == me_e * EXP_DEV + i
            load_ref[i] = jnp.sum(jnp.where(hit, load, 0.0))
            energy_ref[i] = jnp.sum(jnp.where(hit, ratio, 0.0))

    tasks = [lambda: stats_store(0, stats), lambda: stats_send(0)]
    for n in range(1, 4):
        tasks.append(functools.partial(lambda n: stats_store(n, stats_sum(n - 1)), n))
        tasks.append(functools.partial(stats_send, n))
    tasks.append(lambda: stats_out(stats_sum(3)))

    def next_task():
        if tasks:
            tasks.pop(0)()

    next_task()

    @pl.when(active)
    def _():
        recv1[me_e] = send1[zl, :, cols(kme)]
        wait(recv1.at[pl.ds(0, NS - 1)], s1_recv)

        @pl.loop(0, NS)
        def _(j):
            send2[j] = recv1[tgt_ref[j]]

        xbuf[p, y, :, cols(kme)] = recv1[tgt_ref[me_e]]

        @pl.loop(1, NZ * NXC)
        def _(q):
            t = q // NXC
            z = (p + ((t + 1) // 2) * (2 * (t % 2) - 1) + NZ) % NZ
            xct = (xc + q) % NXC
            remote(
                send2.at[(z % ZL) * NXC + xct], xbuf.at[p, y, :, cols(kme)], s2_send, s2_recv.at[p], dev(z, y, xct)
            )

    offs = [((t + 1) // 2) * (2 * (t % 2) - 1) for t in range(NZ)]
    slot = tgt_ref[me_e]
    slot_z = slot // NXC
    ynext, yprev, yopp = (y + 1) % Y, (y + Y - 1) % Y, (y + 2) % Y

    def ring(i):
        return (p + offs[i] + NZ) % NZ

    def own_group(i):
        r = ring(i)
        if offs[i] == 0:
            @pl.when(active)
            def _():
                if KP > 1:
                    wait(xbuf.at[r, y, :, pl.ds(0, CW - PC)], s2_recv.at[r])

            @pl.when(jnp.logical_not(active))
            def _():
                wait(xbuf.at[r, y], s2_recv.at[r])
        else:
            wait(xbuf.at[r, y], s2_recv.at[r])
        remote(xbuf.at[r, y], xbuf.at[r, y], y_send, yp_recv.at[i], dev(p, ynext, xc))
        remote(xbuf.at[r, y], xbuf.at[r, y], y_send, ym_recv.at[i], dev(p, yprev, xc))

    def forward(i):
        r = ring(i)
        if i % 2 == 0:
            wait(xbuf.at[r, yprev], yp_recv.at[i])
            remote(xbuf.at[r, yprev], xbuf.at[r, yprev], y_send, yf_recv.at[i], dev(p, ynext, xc))
        else:
            wait(xbuf.at[r, ynext], ym_recv.at[i])
            remote(xbuf.at[r, ynext], xbuf.at[r, ynext], y_send, yf_recv.at[i], dev(p, yprev, xc))

    def arrived(i):
        r = ring(i)
        if i % 2 == 0:
            wait(xbuf.at[r, ynext], ym_recv.at[i])
        else:
            wait(xbuf.at[r, yprev], yp_recv.at[i])
        wait(xbuf.at[r, yopp], yf_recv.at[i])

    pairs = []
    for a in range(NZ):
        for b in range(a + 1, NZ):
            if (offs[a] - offs[b]) % NZ == ZL:
                pairs.append((b, a))
    pairs.sort()
    first = [True]

    def project(a, b):
        arrived(a)
        arrived(b)
        m = ring(a) % ZL
        near = half(m, slot_z) == 0
        lhs = jnp.concatenate([xbuf[m].reshape(Y * rows, CW), xbuf[m + ZL].reshape(Y * rows, CW)], axis=0)
        opening = first[0]
        first[0] = False
        if opening:
            wait(gate_v, w_sem)
            wait(up_v, w_sem)
            wait(down_v, w_sem)
        for weight, acc in ((gate_v, gacc), (up_v, uacc)):
            value = jnp.dot(lhs, weight[m], preferred_element_type=F32)
            a, b = value[: Y * rows], value[Y * rows :]
            for h, part in ((0, jnp.where(near, a, b)), (1, jnp.where(near, b, a))):
                if opening:
                    acc[h] = part
                else:
                    acc[h] += part

    for i in range(NZ):
        own_group(i)
        if i >= 1:
            forward(i - 1)
            next_task()
        if pairs and pairs[0][0] + 2 <= i:
            b, a = pairs.pop(0)
            project(a, b)
    forward(NZ - 1)
    for b, a in pairs:
        project(a, b)

    g = gacc[...]
    hid[...] = (g / (1.0 + jnp.exp(-g)) * uacc[...]).astype(BF16)

    def back(i):
        return ring(NZ - 1 - i)

    def sign(i):
        return (ynext, yprev) if i % 2 == 0 else (yprev, ynext)

    def compute(i):
        r = back(i)
        value = jnp.dot(hid[half(r, slot_z)], down_v[r % ZL], preferred_element_type=F32)
        pbuf[i] = value.astype(BF16).reshape(Y, rows, CW)

    def send_parts(i):
        to, other = sign(i)
        remote(pbuf.at[i, yopp], ra.at[i], r_send, ra_recv.at[i], dev(p, to, xc))
        remote(pbuf.at[i, other], rb.at[i, 0], r_send, rb0_recv.at[i], dev(p, other, xc))

    def add_passing(i):
        to, _ = sign(i)
        wait(ra.at[i], ra_recv.at[i])
        bs[i] = (pbuf[i, to].astype(F32) + ra[i].astype(F32)).astype(BF16)

    def send_passing(i):
        to, _ = sign(i)
        remote(bs.at[i], rb.at[i, 1], r_send, rb1_recv.at[i], dev(p, to, xc))

    def add_own(i):
        wait(rb.at[i, 0], rb0_recv.at[i])
        wait(rb.at[i, 1], rb1_recv.at[i])
        sz[i] = (pbuf[i, y].astype(F32) + rb[i, 0].astype(F32) + rb[i, 1].astype(F32)).astype(BF16)

    def send_relays(i):
        r = back(i)
        m = r % ZL
        mine_here = offs[NZ - 1 - i] == 0

        @pl.loop(0, KP)
        def _(kk):
            k = (kk + xc) % KP
            xct = (k + C * m) % NXC

            def go():
                remote(sz.at[i, :, cols(k)], zr.at[mine], z_send, zr_recv, dev(r, y, xct))

            if mine_here:
                pl.when(xct != xc)(go)
            else:
                go()

    compute(0)
    for i in range(NZ + 2):
        if i + 1 < NZ:
            compute(i + 1)
        if i < NZ:
            send_parts(i)
        if 1 <= i <= NZ:
            add_passing(i - 1)
        if i >= 2:
            add_own(i - 2)
        if 1 <= i <= NZ:
            send_passing(i - 1)
        next_task()
        if i >= 2:
            send_relays(i - 2)
    while tasks:
        next_task()

    @pl.when(active)
    def _():
        zr[mine] = sz[NZ - 1, :, cols(kme)]
        wait(zr.at[pl.ds(0, NZ * NXC - 1)], zr_recv)

        @pl.loop(0, NS)
        def _(s):
            j = src_ref[s]
            f1[s] = (zr[j].astype(F32) + zr[j + NS].astype(F32)).astype(BF16)

        fin[:, pl.ds(pl.multiple_of(zl * CW + kme * PC, PC), PC)] = f1[me_e]

        @pl.loop(1, NS)
        def _(i):
            s = (me_e + i) % NS
            s_z = s // NXC
            remote(
                f1.at[s],
                fin.at[:, pl.ds(pl.multiple_of(zl * CW + kme * PC, PC), PC)],
                f_send,
                f_recv,
                dev(ZL * half(p, s_z) + s_z, y, s % NXC),
            )

        wait(send2.at[pl.ds(0, ZL * KP - 1)], f_recv)

    @pl.when(jnp.logical_not(active))
    def _():
        wait(fin, f_recv)

    copy_out = pltpu.make_async_copy(fin, out_hbm, in_sem)
    copy_out.start()

    @pl.when(active)
    def _():
        wait(zr.at[pl.ds(0, ZL * KP - 1)], s1_send)
        wait(zr.at[pl.ds(0, NZ * NXC - 1)], s2_send)
        wait(zr.at[pl.ds(0, NZ * KP - 1)], z_send)
        wait(zr.at[pl.ds(0, NS - 1)], f_send)

    @pl.when(jnp.logical_not(active))
    def _():
        wait(zr.at[pl.ds(0, ZL * KP)], s1_send)
        wait(zr.at[pl.ds(0, NZ * KP)], z_send)

    wait(pbuf.at[pl.ds(0, 3 * NZ // Y)], y_send)
    wait(pbuf.at[pl.ds(0, 3 * NZ // Y)], r_send)
    copy_out.wait()


def on_device(L, tokens, routed, expert_ids, norm_gain, gate_weight, up_weight, down_weight, old_place, new_place, probe_ids):
    slot_index = jnp.arange(L.NS, dtype=jnp.int32)
    matches = new_place[:, None] == old_place[None, :]
    sources = jnp.sum(jnp.where(matches, slot_index[None, :], 0), axis=1)
    targets = jnp.sum(jnp.where(matches, slot_index[:, None], 0), axis=0)
    NZ, NXC, Y, ZL, KP, NS, CW, rows = L.NZ, L.NXC, L.Y, L.ZL, L.KP, L.NS, L.CW, L.ROWS
    smem = pl.BlockSpec(memory_space=pltpu.SMEM)
    vmem = pl.BlockSpec(memory_space=pltpu.VMEM)
    anyspace = pl.BlockSpec(memory_space=pl.ANY)
    dma = pltpu.SemaphoreType.DMA
    V = pltpu.VMEM
    scratch = [
        V((L.TOKS, L.D), BF16), V((L.D // 128, 128), F32),
        V((ZL, CW, L.HID), BF16), V((ZL, CW, L.HID), BF16), V((ZL, L.HID, CW), BF16),
        V((ZL, rows, CW), BF16), V((NS, rows, PC), BF16), V((NS, rows, PC), BF16),
        V((NZ, Y, rows, CW), BF16),
        V((L.ZH, Y * rows, L.HID), F32), V((L.ZH, Y * rows, L.HID), F32), V((L.ZH, Y * rows, L.HID), BF16),
        V((NZ, Y, rows, CW), BF16), V((NZ, rows, CW), BF16), V((NZ, 2, rows, CW), BF16),
        V((NZ, rows, CW), BF16), V((NZ, rows, CW), BF16),
        V((NZ * NXC, rows, PC), BF16), V((NS, rows, PC), BF16), V((rows, L.D), BF16),
        V((Y, 8, 128), F32), V((NZ, 8, 128), F32), V((L.X, 8, 128), F32), V((L.C, 8, 128), F32),
        dma, dma, dma, dma, dma, dma((NZ,)), dma, dma((NZ,)), dma((NZ,)), dma((NZ,)),
        dma, dma((NZ,)), dma((NZ,)), dma((NZ,)), dma, dma, dma, dma, dma((4,)), dma((4,)),
    ]
    return pl.pallas_call(
        functools.partial(kernel, L, tokens),
        out_shape=(
            jax.ShapeDtypeStruct((EXP_DEV,), F32),
            jax.ShapeDtypeStruct((EXP_DEV,), F32),
            jax.ShapeDtypeStruct((rows, L.D), BF16),
        ),
        in_specs=[smem, smem, smem, vmem, vmem, anyspace, anyspace, anyspace, anyspace],
        out_specs=(smem, smem, anyspace),
        scratch_shapes=scratch,
        compiler_params=pltpu.CompilerParams(
            collective_id=0, has_side_effects=True, vmem_limit_bytes=60 * 1024 * 1024
        ),
        name="probe_pass",
    )(
        targets, sources, probe_ids, expert_ids.T, norm_gain.reshape(L.D // 128, 128),
        routed, gate_weight[0], up_weight[0], down_weight[0],
    )


def build(mesh, L, tokens):
    both = ("dp", "expert")
    return jax.shard_map(
        functools.partial(on_device, L, tokens),
        mesh=mesh,
        in_specs=(
            P(both, None), P(both, None), P(), P("expert", None, "dp"), P("expert", None, "dp"),
            P("expert", "dp", None), P(), P(), P(both),
        ),
        out_specs=(P("expert"), P("expert"), P(both, None)),
        check_vma=False,
    )


def solution(mesh):
    L = Layout()
    return build(mesh, L, L.TOKS * L.ZH * L.Y * L.NS)
```

```python
import functools

import jax
import jax.numpy as jnp
from jax import lax
from jax.experimental import pallas as pl
from jax.experimental.pallas import tpu as pltpu
from jax.sharding import PartitionSpec as P

MESH = pl.DeviceIdType.MESH
F32 = jnp.float32
BF16 = jnp.bfloat16
EXP_DEV = 8
TOP = 8
EPS = 1e-06
PC = 256
LAG = 3
BACK_LAG = 3
LAST_LAG = 2


class Layout:
    def __init__(self, zh=2, y=4, zl=4, x=4, c=2, pieces=7, rows=40, toks=128, hid=256):
        self.ZH, self.Y, self.ZL, self.X, self.C = zh, y, zl, x, c
        self.KP, self.ROWS, self.TOKS, self.HID = pieces, rows, toks, hid
        self.NZ, self.NXC = zh * zl, x * c
        self.NS = zl * x * c
        self.CW = pieces * PC
        self.D = zl * self.CW
        head = rows * 2 // 5 // 8 * 8 or rows // 2
        self.PARTS = ((0, head), (head, rows - head))


def kernel(
    L, tokens,
    old_ref, new_ref, pid_ref, ids_ref, gain_ref, routed_hbm, gate_hbm, up_hbm, down_hbm,
    stats_hbm, out_hbm,
    routed_v, gain_v, gate_v, up_v, down_v,
    send1, recv1_a, recv1_b, send2_a, send2_b, xbuf, gacc, uacc, hid,
    pbuf, ra, rb, bs, sz, zr_a, zr_b, f1_a, f1_b, fin,
    st_y, st_z, st_x, st_c, st_out, tgt_ref, src_ref,
    in_sem, w_sem, s1_send, s1_recv, s2_send, s2_recv, y_send, yp_recv, ym_recv, yf_recv,
    r_send, ra_recv, rb0_recv, rb1_recv, z_send, zr_recv, f_send, f_recv, st_send, st_recv, st_sem,
):
    Y, ZL, X, C, KP, NZ, NXC, NS, CW = L.Y, L.ZL, L.X, L.C, L.KP, L.NZ, L.NXC, L.NS, L.CW
    rows = L.ROWS
    PARTS = L.PARTS
    recv1, send2, zr, f1 = (recv1_a, recv1_b), (send2_a, send2_b), (zr_a, zr_b), (f1_a, f1_b)
    me_d, me_e = lax.axis_index("dp"), lax.axis_index("expert")
    div, rem = lax.div, lax.rem
    zh, y = div(me_d, Y), rem(me_d, Y)
    zl, xc = div(me_e, NXC), rem(me_e, NXC)
    x, c = div(xc, C), rem(xc, C)
    p = zh * ZL + zl
    kme = rem(xc - C * zl + C * NXC, NXC)
    active = kme < KP
    mine = p * NXC + xc
    offs = [((t + 1) // 2) * (2 * (t % 2) - 1) for t in range(NZ)]
    REACH = ZL // 2
    zs = [rem(p + o + NZ, NZ) for o in offs]
    xcs = [rem(xc + q, NXC) for q in range(NXC)]

    def dev(z, yy, xcc):
        return (div(z, ZL) * Y + yy, rem(z, ZL) * NXC + xcc)

    def half(r, z_low):
        return div(rem(r - z_low + ZL // 2 - 1 + rem(r, 2) + NZ, NZ), ZL)

    def span(part):
        return pl.ds(*PARTS[part])

    def cols(k):
        return pl.ds(pl.multiple_of(k * PC, PC), PC)

    def remote(src, dst, send, recv, where):
        pltpu.make_async_remote_copy(
            src_ref=src, dst_ref=dst, send_sem=send, recv_sem=recv, device_id=where, device_id_type=MESH
        ).start()

    def wait(ref, sem):
        pltpu.make_async_copy(ref, ref, sem).wait()

    copy_in = pltpu.make_async_copy(routed_hbm, routed_v, in_sem)
    copy_in.start()
    barrier = pltpu.get_barrier_semaphore()

    for t in reversed(range(NZ)):
        for q in reversed(range(NXC)):
            if (t or q) and abs(offs[t]) <= REACH:
                pl.semaphore_signal(barrier, inc=1, device_id=dev(zs[t], y, xcs[q]), device_id_type=MESH)
    for dy in range(1, Y):
        pl.semaphore_signal(barrier, inc=1, device_id=dev(p, rem(y + dy, Y), xc), device_id_type=MESH)

    gain_v[...] = gain_ref[...].astype(F32)
    lane = lax.broadcasted_iota(jnp.int32, (8, L.TOKS), 1)
    sub = lax.broadcasted_iota(jnp.int32, (8, L.TOKS), 0)
    picks = []
    for b in range(rows // 8):
        want = jnp.zeros((8, L.TOKS), jnp.int32)
        for i in range(8):
            want = jnp.where(sub == i, pid_ref[b * 8 + i], want)
        picks.append((lane == want).astype(F32))
    select = jnp.concatenate(picks, axis=0).astype(BF16)

    copy_in.wait()
    for hbm, v in ((gate_hbm, gate_v), (up_hbm, up_v)):
        for m in range(ZL):
            pltpu.make_async_copy(hbm.at[pl.ds(m * CW, CW), :], v.at[m], w_sem).start()
    for m in range(ZL):
        pltpu.make_async_copy(down_hbm.at[:, pl.ds(m * CW, CW)], down_v.at[m], w_sem).start()

    square = jnp.zeros((rows, 1), F32)
    for m in range(ZL):
        picked = jnp.dot(select, routed_v[:, m * CW : (m + 1) * CW], preferred_element_type=F32)
        square += jnp.sum(picked * picked, axis=1, keepdims=True)
        send1[m] = picked.astype(BF16)
    scale = lax.rsqrt(square / L.D + EPS)
    for m in range(ZL):
        for t in range(CW // 128):
            tile = m * (CW // 128) + t
            v = send1[m, :, t * 128 : (t + 1) * 128].astype(F32)
            send1[m, :, t * 128 : (t + 1) * 128] = (v * scale * gain_v[tile : tile + 1, :]).astype(BF16)

    pl.semaphore_wait(barrier, sum(abs(o) <= REACH for o in offs) * NXC - 1 + Y - 1)

    near = [(m, m + ZL * rem(half(m, zl) + zh, 2)) for m in range(ZL)]
    def to_relays(part):
        for n in range(KP):
            k = rem(xc + n, KP)
            for m, r in near:
                xct = rem(k + C * m, NXC)

                @pl.when(r * NXC + xct != mine)
                def _():
                    remote(
                        send1.at[m, span(part), cols(k)], recv1[part].at[me_e], s1_send, s1_recv.at[part],
                        dev(r, y, xct),
                    )

    to_relays(0)

    def find(out, values, among):
        @pl.loop(0, NS)
        def _(i):
            value = values[i]
            found = 0
            for j in range(NS):
                found = jnp.where(among[j] == value, j, found)
            out[i] = found

    find(tgt_ref, old_ref, new_ref)
    find(src_ref, new_ref, old_ref)

    def squares(i, acc):
        v = routed_v[:, pl.ds(pl.multiple_of(i * PC, PC), PC)].astype(F32)
        return acc + v * v

    total = lax.fori_loop(0, L.D // PC, squares, jnp.zeros((L.TOKS, PC), F32))
    mean_square = jnp.sum(total, axis=1, keepdims=True) / L.D
    ids = ids_ref[...].astype(F32).T
    expert = lax.broadcasted_iota(jnp.int32, (L.TOKS, 256), 1).astype(F32)
    onehot = jnp.zeros((L.TOKS, 256), F32)
    for k in range(TOP):
        onehot += (ids[:, k : k + 1] == expert).astype(F32)
    counts = jnp.sum(onehot, axis=0, keepdims=True)
    energy = jnp.sum(onehot * mean_square, axis=0, keepdims=True)
    stats = jnp.concatenate(
        [counts[:, :128], counts[:, 128:], energy[:, :128], energy[:, 128:], jnp.zeros((4, 128), F32)], axis=0
    )
    rounds = (
        (st_y, Y, y, lambda o: dev(p, o, xc)),
        (st_z, NZ, p, lambda o: dev(o, y, xc)),
        (st_x, X, x, lambda o: dev(p, y, o * C + c)),
        (st_c, C, c, lambda o: dev(p, y, x * C + o)),
    )

    def stats_store(n, value):
        buf, _, own, _ = rounds[n]
        buf[own] = value

    def stats_send(n):
        buf, size, own, where = rounds[n]
        for step in range(1, size):
            remote(buf.at[own], buf.at[own], st_send.at[n], st_recv.at[n], where(rem(own + step, size)))

    def stats_sum(n):
        buf, size, own, _ = rounds[n]
        if size > 1:
            wait(buf.at[pl.ds(0, size - 1)], st_recv.at[n])
            wait(buf.at[pl.ds(0, size - 1)], st_send.at[n])
        value = buf[0]
        for o in range(1, size):
            value += buf[o]
        return value

    def stats_out(value):
        where = lax.broadcasted_iota(jnp.int32, (2, 128), 0) * 128 + lax.broadcasted_iota(jnp.int32, (2, 128), 1)
        row, col = lax.broadcasted_iota(jnp.int32, (8, 128), 0), lax.broadcasted_iota(jnp.int32, (8, 128), 1)
        tile = jnp.zeros((8, 128), F32)
        for i in range(EXP_DEV):
            hit = where == me_e * EXP_DEV + i
            for n in range(2):
                one = jnp.sum(jnp.where(hit, value[2 * n : 2 * n + 2], 0.0))
                tile = jnp.where((row == n) & (col == i), one, tile)
        st_out[...] = tile
        pltpu.make_async_copy(st_out, stats_hbm, st_sem).start()

    def stats_next(n):
        stats_store(n, stats_sum(n - 1))

    stats_store(0, stats)
    to_relays(1)

    def relay(part):
        @pl.when(active)
        def _():
            got, put = recv1[part], send2[part]
            got[me_e] = send1[zl, span(part), cols(kme)]
            wait(got.at[pl.ds(0, NS - 1)], s1_recv.at[part])
            for j in range(NS):
                put[j] = got[tgt_ref[j]]
            xbuf[p, y, span(part), cols(kme)] = got[tgt_ref[me_e]]

    def to_holders(part, ts):
        @pl.when(active)
        def _():
            for t in ts:
                for q in range(NXC):
                    if t or q:
                        remote(
                            send2[part].at[rem(zs[t], ZL) * NXC + xcs[q]],
                            xbuf.at[p, y, span(part), cols(kme)],
                            s2_send.at[part],
                            s2_recv.at[part * NZ + p],
                            dev(zs[t], y, xcs[q]),
                        )

    slot = tgt_ref[me_e]
    slot_z = div(slot, NXC)
    ynext, yprev, yopp = rem(y + 1, Y), rem(y + Y - 1, Y), rem(y + 2, Y)

    pairs = []
    for a in range(NZ):
        for b in range(a + 1, NZ):
            if (offs[a] - offs[b]) % NZ == ZL:
                pairs.append((b, a))
    pairs.sort()
    orders = (list(range(NZ)), [i for b, a in pairs[:-1] for i in (a, b)] + list(pairs[-1]))

    def place(u):
        return u // NZ, orders[u // NZ][u % NZ]

    def ring(i):
        return zs[i]

    def block(u, who):
        part, i = place(u)
        return xbuf.at[ring(i), who, span(part)]

    def own_group(u):
        part, i = place(u)
        mine_here = block(u, y)
        sem = s2_recv.at[part * NZ + ring(i)]
        if offs[i] == 0:
            @pl.when(active)
            def _():
                if KP > 1:
                    wait(xbuf.at[p, y, span(part), pl.ds(0, CW - PC)], sem)

            @pl.when(jnp.logical_not(active))
            def _():
                wait(mine_here, sem)
        else:
            wait(mine_here, sem)
        remote(mine_here, mine_here, y_send, yp_recv.at[u], dev(p, ynext, xc))
        remote(mine_here, mine_here, y_send, ym_recv.at[u], dev(p, yprev, xc))

    def forward(u):
        if u % 2 == 0:
            wait(block(u, yprev), yp_recv.at[u])
            remote(block(u, yprev), block(u, yprev), y_send, yf_recv.at[u], dev(p, ynext, xc))
        else:
            wait(block(u, ynext), ym_recv.at[u])
            remote(block(u, ynext), block(u, ynext), y_send, yf_recv.at[u], dev(p, yprev, xc))

    def arrived(u):
        if u % 2 == 0:
            wait(block(u, ynext), ym_recv.at[u])
        else:
            wait(block(u, yprev), yp_recv.at[u])
        wait(block(u, yopp), yf_recv.at[u])

    first = [True]

    def project(a, b):
        for i in (a, b):
            arrived(i)
            arrived(NZ + orders[1].index(i))
        m = rem(ring(a), ZL)
        near = half(m, slot_z) == 0
        lhs = jnp.concatenate([xbuf[m].reshape(Y * rows, CW), xbuf[m + ZL].reshape(Y * rows, CW)], axis=0)
        opening = first[0]
        first[0] = False
        if opening:
            wait(gate_v, w_sem)
            wait(up_v, w_sem)
            wait(down_v, w_sem)
        for weight, acc in ((gate_v, gacc), (up_v, uacc)):
            value = jnp.dot(lhs, weight[m], preferred_element_type=F32)
            a, b = value[: Y * rows], value[Y * rows :]
            for h, part in ((0, jnp.where(near, a, b)), (1, jnp.where(near, b, a))):
                if opening:
                    acc[h] = part
                else:
                    acc[h] += part

    units = 2 * NZ
    relay(0)
    to_holders(0, range(NZ))
    stats_send(0)
    own_group(0)
    relay(1)
    to_holders(1, orders[1][: NZ // 2])
    for u in range(1, units):
        own_group(u)
        if u - 1 in range(NZ // 2):
            to_holders(1, orders[1][NZ // 2 + u - 1 : NZ // 2 + u])
        if u >= LAG:
            forward(u - LAG)
        if u == units // 4:
            stats_next(1)
        if u == units // 4 + 1:
            stats_send(1)
        if u == units - 3:
            stats_next(2)
        if u == units - 2:
            stats_send(2)
    for u in range(units - LAG, units):
        forward(u)
        if u < units - 1 and len(pairs) > 2:
            project(*pairs.pop(0)[::-1])
    for b, a in pairs:
        project(a, b)

    g = gacc[...]
    hid[...] = (g / (1.0 + jnp.exp(-g)) * uacc[...]).astype(BF16)

    def back(i):
        return ring(NZ - 1 - i)

    def sign(i):
        return (ynext, yprev) if i % 2 == 0 else (yprev, ynext)

    def compute(i):
        r = back(i)
        value = jnp.dot(hid[half(r, slot_z)], down_v[rem(r, ZL)], preferred_element_type=F32)
        pbuf[i] = value.astype(BF16).reshape(Y, rows, CW)

    def unit(v):
        return 1 - v // NZ, v % NZ

    def send_parts(v):
        part, i = unit(v)
        to, _ = sign(v)
        remote(pbuf.at[i, yopp, span(part)], ra.at[i, span(part)], r_send, ra_recv.at[v], dev(p, to, xc))

    def add_passing(v):
        part, i = unit(v)
        to, _ = sign(v)
        wait(ra.at[i, span(part)], ra_recv.at[v])
        bs[i, span(part)] = (pbuf[i, to, span(part)].astype(F32) + ra[i, span(part)].astype(F32)).astype(BF16)

    def send_passing(v):
        part, i = unit(v)
        to, other = sign(v)
        remote(bs.at[i, span(part)], rb.at[i, 1, span(part)], r_send, rb1_recv.at[v], dev(p, to, xc))
        remote(pbuf.at[i, other, span(part)], rb.at[i, 0, span(part)], r_send, rb0_recv.at[v], dev(p, other, xc))

    def add_own(v):
        part, i = unit(v)
        rw = span(part)
        wait(rb.at[i, 0, rw], rb0_recv.at[v])
        wait(rb.at[i, 1, rw], rb1_recv.at[v])
        sz[i, rw] = (pbuf[i, y, rw].astype(F32) + rb[i, 0, rw].astype(F32) + rb[i, 1, rw].astype(F32)).astype(BF16)

    def send_relays(v):
        part, i = unit(v)
        r = back(i)
        m = rem(r, ZL)
        for n in range(KP):
            k = rem(xc + n, KP)
            xct = rem(k + C * m, NXC)

            def go():
                remote(
                    sz.at[i, span(part), cols(k)], zr[part].at[mine], z_send.at[part], zr_recv.at[part], dev(r, y, xct)
                )

            if offs[NZ - 1 - i] == 0:
                pl.when(xct != xc)(go)
            else:
                go()

    chunk = pl.ds(pl.multiple_of(zl * CW + kme * PC, PC), PC)

    def relay_back(part):
        @pl.when(active)
        def _():
            got, put = zr[part], f1[part]
            got[mine] = sz[NZ - 1, span(part), cols(kme)]
            wait(got.at[pl.ds(0, NZ * NXC - 1)], zr_recv.at[part])
            for s in range(NS):
                j = src_ref[s]
                put[s] = (got[j].astype(F32) + got[j + NS].astype(F32)).astype(BF16)
            fin[span(part), chunk] = put[me_e]

            for n in range(ZL):
                s_z = rem(zl + n, ZL)
                z = ZL * half(p, s_z) + s_z
                for q in range(NXC):
                    if n or q:
                        remote(
                            put.at[s_z * NXC + xcs[q]], fin.at[span(part), chunk], f_send.at[part], f_recv.at[part],
                            dev(z, y, xcs[q]),
                        )

    compute(0)
    for v in range(units + BACK_LAG + LAST_LAG):
        if v < units:
            send_parts(v)
        passing = v - BACK_LAG
        if 0 <= passing < units:
            add_passing(passing)
        if v + 1 < NZ:
            compute(v + 1)
        if 0 <= passing < units:
            send_passing(passing)
        done = v - BACK_LAG - LAST_LAG
        if done >= 0:
            add_own(done)
            if done == 2:
                stats_next(3)
            if done == 3:
                stats_send(3)
            if done == NZ + 1:
                stats_out(stats_sum(3))
            send_relays(done)
            if done == NZ + 3:
                relay_back(1)
    relay_back(0)

    def returned(part):
        @pl.when(active)
        def _():
            wait(send2[part].at[pl.ds(0, ZL * KP - 1)], f_recv.at[part])

        @pl.when(jnp.logical_not(active))
        def _():
            wait(send2[part].at[pl.ds(0, ZL * KP)], f_recv.at[part])

    returned(1)
    returned(0)
    copy_out = pltpu.make_async_copy(fin, out_hbm, in_sem)
    copy_out.start()

    @pl.when(active)
    def _():
        wait(send1.at[pl.ds(0, ZL - 1)], s1_send)
        if KP > 1:
            wait(send1.at[0, :, pl.ds(0, CW - PC)], s1_send)
        for part in range(2):
            wait(zr[part].at[pl.ds(0, NZ * NXC - 1)], s2_send.at[part])
            wait(zr[part].at[pl.ds(0, NZ * KP - 1)], z_send.at[part])
            wait(zr[part].at[pl.ds(0, NS - 1)], f_send.at[part])

    @pl.when(jnp.logical_not(active))
    def _():
        wait(send1, s1_send)
        for part in range(2):
            wait(zr[part].at[pl.ds(0, NZ * KP)], z_send.at[part])

    wait(pbuf.at[pl.ds(0, 3 * NZ // Y)], y_send)
    wait(pbuf.at[pl.ds(0, 3 * NZ // Y)], r_send)
    pltpu.make_async_copy(st_out, stats_hbm, st_sem).wait()
    copy_out.wait()


def on_device(L, tokens, routed, expert_ids, norm_gain, gate_weight, up_weight, down_weight, old_place, new_place, probe_ids):
    NZ, NXC, Y, ZL, KP, NS, CW, rows = L.NZ, L.NXC, L.Y, L.ZL, L.KP, L.NS, L.CW, L.ROWS
    smem = pl.BlockSpec(memory_space=pltpu.SMEM)
    vmem = pl.BlockSpec(memory_space=pltpu.VMEM)
    anyspace = pl.BlockSpec(memory_space=pl.ANY)
    dma = pltpu.SemaphoreType.DMA
    V = pltpu.VMEM

    def pieces(n):
        return [V((n, size, PC), BF16) for _, size in L.PARTS]

    scratch = [
        V((L.TOKS, L.D), BF16), V((L.D // 128, 128), F32),
        V((ZL, CW, L.HID), BF16), V((ZL, CW, L.HID), BF16), V((ZL, L.HID, CW), BF16),
        V((ZL, rows, CW), BF16), *pieces(NS), *pieces(NS),
        V((NZ, Y, rows, CW), BF16),
        V((L.ZH, Y * rows, L.HID), F32), V((L.ZH, Y * rows, L.HID), F32), V((L.ZH, Y * rows, L.HID), BF16),
        V((NZ, Y, rows, CW), BF16), V((NZ, rows, CW), BF16), V((NZ, 2, rows, CW), BF16),
        V((NZ, rows, CW), BF16), V((NZ, rows, CW), BF16),
        *pieces(NZ * NXC), *pieces(NS), V((rows, L.D), BF16),
        V((Y, 8, 128), F32), V((NZ, 8, 128), F32), V((L.X, 8, 128), F32), V((L.C, 8, 128), F32), V((8, 128), F32),
        pltpu.SMEM((NS,), jnp.int32), pltpu.SMEM((NS,), jnp.int32),
        dma, dma, dma, dma((2,)), dma((2,)), dma((2 * NZ,)), dma, dma((2 * NZ,)), dma((2 * NZ,)), dma((2 * NZ,)),
        dma, dma((2 * NZ,)), dma((2 * NZ,)), dma((2 * NZ,)), dma((2,)), dma((2,)), dma((2,)), dma((2,)), dma((4,)), dma((4,)), dma,
    ]
    stats, probe_out = pl.pallas_call(
        functools.partial(kernel, L, tokens),
        out_shape=(
            jax.ShapeDtypeStruct((8, 128), F32),
            jax.ShapeDtypeStruct((rows, L.D), BF16),
        ),
        in_specs=[smem, smem, smem, vmem, vmem, anyspace, anyspace, anyspace, anyspace],
        out_specs=(anyspace, anyspace),
        scratch_shapes=scratch,
        compiler_params=pltpu.CompilerParams(
            collective_id=0, has_side_effects=True, vmem_limit_bytes=60 * 1024 * 1024
        ),
        name="probe_pass",
    )(
        old_place, new_place, probe_ids, expert_ids.T, norm_gain.reshape(L.D // 128, 128),
        routed, gate_weight[0], up_weight[0], down_weight[0],
    )
    counts, energy = stats[0, :EXP_DEV], stats[1, :EXP_DEV]
    return counts * (EXP_DEV * NS) / (tokens * TOP), energy / counts, probe_out


def build(mesh, L, tokens):
    both = ("dp", "expert")
    return jax.shard_map(
        functools.partial(on_device, L, tokens),
        mesh=mesh,
        in_specs=(
            P(both, None), P(both, None), P(), P("expert", None, "dp"), P("expert", None, "dp"),
            P("expert", "dp", None), P(), P(), P(both),
        ),
        out_specs=(P("expert"), P("expert"), P(both, None)),
        check_vma=False,
    )


def solution(mesh):
    L = Layout()
    return build(mesh, L, L.TOKS * L.ZH * L.Y * L.NS)
```

```python
import functools

import jax
import jax.numpy as jnp
from jax import lax
from jax.experimental import pallas as pl
from jax.experimental.pallas import tpu as pltpu
from jax.sharding import PartitionSpec as P

MESH = pl.DeviceIdType.MESH
F32 = jnp.float32
BF16 = jnp.bfloat16
EXP_DEV = 8
TOP = 8
EPS = 1e-06
PC = 256
LAG = 2
BACK_LAG = 3
LAST_LAG = 2


class Layout:
    def __init__(self, zh=2, y=4, zl=4, x=4, c=2, pieces=7, rows=40, toks=128, hid=256):
        self.ZH, self.Y, self.ZL, self.X, self.C = zh, y, zl, x, c
        self.KP, self.ROWS, self.TOKS, self.HID = pieces, rows, toks, hid
        self.NZ, self.NXC = zh * zl, x * c
        self.NS = zl * x * c
        self.CW = pieces * PC
        self.D = zl * self.CW
        head = rows * 2 // 5 // 8 * 8 or rows // 2
        self.PARTS = ((0, head), (head, rows - head))


def kernel(
    L, tokens,
    old_ref, new_ref, pid_ref, ids_ref, gain_ref, routed_hbm, gate_hbm, up_hbm, down_hbm,
    stats_hbm, out_hbm,
    routed_v, gain_v, gate_v, up_v, down_v,
    send1, recv1_a, recv1_b, send2_a, send2_b, xbuf, gacc, uacc, hid,
    pbuf, ra, rb, bs, sz, zr_a, zr_b, f1_a, f1_b, fin,
    st_y, st_z, st_x, st_c, st_out, tgt_ref, src_ref,
    in_sem, w_sem, s1_send, s1_recv, s2_send, s2_recv, y_send, yp_recv, ym_recv, yf_recv,
    r_send, ra_recv, rb0_recv, rb1_recv, z_send, zr_recv, f_send, f_recv, st_send, st_recv, st_sem,
):
    Y, ZL, X, C, KP, NZ, NXC, NS, CW = L.Y, L.ZL, L.X, L.C, L.KP, L.NZ, L.NXC, L.NS, L.CW
    rows = L.ROWS
    PARTS = L.PARTS
    recv1, send2, zr, f1 = (recv1_a, recv1_b), (send2_a, send2_b), (zr_a, zr_b), (f1_a, f1_b)
    me_d, me_e = lax.axis_index("dp"), lax.axis_index("expert")
    div, rem = lax.div, lax.rem
    zh, y = div(me_d, Y), rem(me_d, Y)
    zl, xc = div(me_e, NXC), rem(me_e, NXC)
    x, c = div(xc, C), rem(xc, C)
    p = zh * ZL + zl
    kme = rem(xc - C * zl + C * NXC, NXC)
    active = kme < KP
    mine = p * NXC + xc
    offs = [((t + 1) // 2) * (2 * (t % 2) - 1) for t in range(NZ)]
    REACH = ZL // 2
    zs = [rem(p + o + NZ, NZ) for o in offs]
    xcs = [rem(xc + q, NXC) for q in range(NXC)]

    def dev(z, yy, xcc):
        return (div(z, ZL) * Y + yy, rem(z, ZL) * NXC + xcc)

    def half(r, z_low):
        return div(rem(r - z_low + ZL // 2 - 1 + rem(r, 2) + NZ, NZ), ZL)

    def span(part):
        return pl.ds(*PARTS[part])

    def cols(k):
        return pl.ds(pl.multiple_of(k * PC, PC), PC)

    def remote(src, dst, send, recv, where):
        pltpu.make_async_remote_copy(
            src_ref=src, dst_ref=dst, send_sem=send, recv_sem=recv, device_id=where, device_id_type=MESH
        ).start()

    def wait(ref, sem):
        pltpu.make_async_copy(ref, ref, sem).wait()

    copy_in = pltpu.make_async_copy(routed_hbm, routed_v, in_sem)
    copy_in.start()
    barrier = pltpu.get_barrier_semaphore()

    for t in reversed(range(NZ)):
        for q in reversed(range(NXC)):
            if (t or q) and abs(offs[t]) <= REACH:
                pl.semaphore_signal(barrier, inc=1, device_id=dev(zs[t], y, xcs[q]), device_id_type=MESH)
    for dy in range(1, Y):
        pl.semaphore_signal(barrier, inc=1, device_id=dev(p, rem(y + dy, Y), xc), device_id_type=MESH)

    gain_v[...] = gain_ref[...].astype(F32)
    lane = lax.broadcasted_iota(jnp.int32, (8, L.TOKS), 1)
    sub = lax.broadcasted_iota(jnp.int32, (8, L.TOKS), 0)
    picks = []
    for b in range(rows // 8):
        want = jnp.zeros((8, L.TOKS), jnp.int32)
        for i in range(8):
            want = jnp.where(sub == i, pid_ref[b * 8 + i], want)
        picks.append((lane == want).astype(F32))
    select = jnp.concatenate(picks, axis=0).astype(BF16)

    copy_in.wait()
    for hbm, v in ((gate_hbm, gate_v), (up_hbm, up_v)):
        for m in range(ZL):
            pltpu.make_async_copy(hbm.at[pl.ds(m * CW, CW), :], v.at[m], w_sem).start()
    for m in range(ZL):
        pltpu.make_async_copy(down_hbm.at[:, pl.ds(m * CW, CW)], down_v.at[m], w_sem).start()

    square = jnp.zeros((rows, 1), F32)
    for m in range(ZL):
        picked = jnp.dot(select, routed_v[:, m * CW : (m + 1) * CW], preferred_element_type=F32)
        square += jnp.sum(picked * picked, axis=1, keepdims=True)
        send1[m] = picked.astype(BF16)
    scale = lax.rsqrt(square / L.D + EPS)
    for m in range(ZL):
        for t in range(CW // 128):
            tile = m * (CW // 128) + t
            v = send1[m, :, t * 128 : (t + 1) * 128].astype(F32)
            send1[m, :, t * 128 : (t + 1) * 128] = (v * scale * gain_v[tile : tile + 1, :]).astype(BF16)

    pl.semaphore_wait(barrier, sum(abs(o) <= REACH for o in offs) * NXC - 1 + Y - 1)

    near = [(m, m + ZL * rem(half(m, zl) + zh, 2)) for m in range(ZL)]
    def to_relays(part):
        for n in range(KP):
            k = rem(xc + n, KP)
            for m, r in near:
                xct = rem(k + C * m, NXC)

                @pl.when(r * NXC + xct != mine)
                def _():
                    remote(
                        send1.at[m, span(part), cols(k)], recv1[part].at[me_e], s1_send, s1_recv.at[part],
                        dev(r, y, xct),
                    )

    to_relays(0)

    def find(out, values, among):
        @pl.loop(0, NS)
        def _(i):
            value = values[i]
            found = 0
            for j in range(NS):
                found = jnp.where(among[j] == value, j, found)
            out[i] = found

    find(tgt_ref, old_ref, new_ref)
    find(src_ref, new_ref, old_ref)

    def squares(i, acc):
        v = routed_v[:, pl.ds(pl.multiple_of(i * PC, PC), PC)].astype(F32)
        return acc + v * v

    total = lax.fori_loop(0, L.D // PC, squares, jnp.zeros((L.TOKS, PC), F32))
    mean_square = jnp.sum(total, axis=1, keepdims=True) / L.D
    ids = ids_ref[...].astype(F32).T
    expert = lax.broadcasted_iota(jnp.int32, (L.TOKS, 256), 1).astype(F32)
    onehot = jnp.zeros((L.TOKS, 256), F32)
    for k in range(TOP):
        onehot += (ids[:, k : k + 1] == expert).astype(F32)
    counts = jnp.sum(onehot, axis=0, keepdims=True)
    energy = jnp.sum(onehot * mean_square, axis=0, keepdims=True)
    stats = jnp.concatenate(
        [counts[:, :128], counts[:, 128:], energy[:, :128], energy[:, 128:], jnp.zeros((4, 128), F32)], axis=0
    )
    rounds = (
        (st_y, Y, y, lambda o: dev(p, o, xc)),
        (st_z, NZ, p, lambda o: dev(o, y, xc)),
        (st_x, X, x, lambda o: dev(p, y, o * C + c)),
        (st_c, C, c, lambda o: dev(p, y, x * C + o)),
    )

    def stats_store(n, value):
        buf, _, own, _ = rounds[n]
        buf[own] = value

    def stats_send(n):
        buf, size, own, where = rounds[n]
        for step in range(1, size):
            remote(buf.at[own], buf.at[own], st_send.at[n], st_recv.at[n], where(rem(own + step, size)))

    def stats_sum(n):
        buf, size, own, _ = rounds[n]
        if size > 1:
            wait(buf.at[pl.ds(0, size - 1)], st_recv.at[n])
            wait(buf.at[pl.ds(0, size - 1)], st_send.at[n])
        value = buf[0]
        for o in range(1, size):
            value += buf[o]
        return value

    def stats_out(value):
        where = lax.broadcasted_iota(jnp.int32, (2, 128), 0) * 128 + lax.broadcasted_iota(jnp.int32, (2, 128), 1)
        row, col = lax.broadcasted_iota(jnp.int32, (8, 128), 0), lax.broadcasted_iota(jnp.int32, (8, 128), 1)
        tile = jnp.zeros((8, 128), F32)
        for i in range(EXP_DEV):
            hit = where == me_e * EXP_DEV + i
            for n in range(2):
                one = jnp.sum(jnp.where(hit, value[2 * n : 2 * n + 2], 0.0))
                tile = jnp.where((row == n) & (col == i), one, tile)
        st_out[...] = tile
        pltpu.make_async_copy(st_out, stats_hbm, st_sem).start()

    def stats_next(n):
        stats_store(n, stats_sum(n - 1))

    stats_store(0, stats)
    to_relays(1)

    def relay(part):
        @pl.when(active)
        def _():
            got, put = recv1[part], send2[part]
            got[me_e] = send1[zl, span(part), cols(kme)]
            wait(got.at[pl.ds(0, NS - 1)], s1_recv.at[part])
            for j in range(NS):
                put[j] = got[tgt_ref[j]]
            xbuf[p, y, span(part), cols(kme)] = got[tgt_ref[me_e]]

    def to_holders(part, ts):
        @pl.when(active)
        def _():
            for t in ts:
                for q in range(NXC):
                    if t or q:
                        remote(
                            send2[part].at[rem(zs[t], ZL) * NXC + xcs[q]],
                            xbuf.at[p, y, span(part), cols(kme)],
                            s2_send.at[part],
                            s2_recv.at[part * NZ + p],
                            dev(zs[t], y, xcs[q]),
                        )

    slot = tgt_ref[me_e]
    slot_z = div(slot, NXC)
    ynext, yprev, yopp = rem(y + 1, Y), rem(y + Y - 1, Y), rem(y + 2, Y)

    pairs = []
    for a in range(NZ):
        for b in range(a + 1, NZ):
            if (offs[a] - offs[b]) % NZ == ZL:
                pairs.append((b, a))
    pairs.sort()
    orders = (list(range(NZ)), list(range(NZ)))

    def place(u):
        return u // NZ, orders[u // NZ][u % NZ]

    def ring(i):
        return zs[i]

    def block(u, who):
        part, i = place(u)
        return xbuf.at[ring(i), who, span(part)]

    def own_group(u):
        part, i = place(u)
        mine_here = block(u, y)
        sem = s2_recv.at[part * NZ + ring(i)]
        if offs[i] == 0:
            @pl.when(active)
            def _():
                if KP > 1:
                    wait(xbuf.at[p, y, span(part), pl.ds(0, CW - PC)], sem)

            @pl.when(jnp.logical_not(active))
            def _():
                wait(mine_here, sem)
        else:
            wait(mine_here, sem)
        remote(mine_here, mine_here, y_send, yp_recv.at[u], dev(p, ynext, xc))
        remote(mine_here, mine_here, y_send, ym_recv.at[u], dev(p, yprev, xc))

    def forward(u):
        if u % 2 == 0:
            wait(block(u, yprev), yp_recv.at[u])
            remote(block(u, yprev), block(u, yprev), y_send, yf_recv.at[u], dev(p, ynext, xc))
        else:
            wait(block(u, ynext), ym_recv.at[u])
            remote(block(u, ynext), block(u, ynext), y_send, yf_recv.at[u], dev(p, yprev, xc))

    def arrived(u):
        if u % 2 == 0:
            wait(block(u, ynext), ym_recv.at[u])
        else:
            wait(block(u, yprev), yp_recv.at[u])
        wait(block(u, yopp), yf_recv.at[u])

    first = [True]

    def project(a, b):
        for i in (a, b):
            arrived(i)
            arrived(NZ + orders[1].index(i))
        m = rem(ring(a), ZL)
        near = half(m, slot_z) == 0
        lhs = jnp.concatenate([xbuf[m].reshape(Y * rows, CW), xbuf[m + ZL].reshape(Y * rows, CW)], axis=0)
        opening = first[0]
        first[0] = False
        if opening:
            wait(gate_v, w_sem)
            wait(up_v, w_sem)
            wait(down_v, w_sem)
        for weight, acc in ((gate_v, gacc), (up_v, uacc)):
            value = jnp.dot(lhs, weight[m], preferred_element_type=F32)
            a, b = value[: Y * rows], value[Y * rows :]
            for h, part in ((0, jnp.where(near, a, b)), (1, jnp.where(near, b, a))):
                if opening:
                    acc[h] = part
                else:
                    acc[h] += part

    units = 2 * NZ
    relay(0)
    to_holders(0, range(NZ))
    stats_send(0)
    own_group(0)
    relay(1)
    to_holders(1, orders[1][: NZ // 2])
    for u in range(1, units):
        own_group(u)
        if u - 1 in range(NZ // 2):
            to_holders(1, orders[1][NZ // 2 + u - 1 : NZ // 2 + u])
        if u >= LAG:
            forward(u - LAG)
        if u == units // 4:
            stats_next(1)
        if u == units // 4 + 1:
            stats_send(1)
        if u == units - 3:
            stats_next(2)
        if u == units - 2:
            stats_send(2)
    for u in range(units - LAG, units):
        forward(u)
        if u < units - 1 and len(pairs) > 2:
            project(*pairs.pop(0)[::-1])
    for b, a in pairs:
        project(a, b)

    g = gacc[...]
    hid[...] = (g / (1.0 + jnp.exp(-g)) * uacc[...]).astype(BF16)

    def back(i):
        return ring(NZ - 1 - i)

    def sign(i):
        return (ynext, yprev) if i % 2 == 0 else (yprev, ynext)

    def compute(i):
        r = back(i)
        value = jnp.dot(hid[half(r, slot_z)], down_v[rem(r, ZL)], preferred_element_type=F32)
        pbuf[i] = value.astype(BF16).reshape(Y, rows, CW)

    def unit(v):
        return 1 - v // NZ, v % NZ

    def send_parts(v):
        part, i = unit(v)
        to, _ = sign(v)
        remote(pbuf.at[i, yopp, span(part)], ra.at[i, span(part)], r_send, ra_recv.at[v], dev(p, to, xc))

    def add_passing(v):
        part, i = unit(v)
        to, _ = sign(v)
        wait(ra.at[i, span(part)], ra_recv.at[v])
        bs[i, span(part)] = (pbuf[i, to, span(part)].astype(F32) + ra[i, span(part)].astype(F32)).astype(BF16)

    def send_passing(v):
        part, i = unit(v)
        to, other = sign(v)
        remote(bs.at[i, span(part)], rb.at[i, 1, span(part)], r_send, rb1_recv.at[v], dev(p, to, xc))
        remote(pbuf.at[i, other, span(part)], rb.at[i, 0, span(part)], r_send, rb0_recv.at[v], dev(p, other, xc))

    def add_own(v):
        part, i = unit(v)
        rw = span(part)
        wait(rb.at[i, 0, rw], rb0_recv.at[v])
        wait(rb.at[i, 1, rw], rb1_recv.at[v])
        sz[i, rw] = (pbuf[i, y, rw].astype(F32) + rb[i, 0, rw].astype(F32) + rb[i, 1, rw].astype(F32)).astype(BF16)

    def send_relays(v):
        part, i = unit(v)
        r = back(i)
        m = rem(r, ZL)
        for n in range(KP):
            k = rem(xc + n, KP)
            xct = rem(k + C * m, NXC)

            def go():
                remote(
                    sz.at[i, span(part), cols(k)], zr[part].at[mine], z_send.at[part], zr_recv.at[part], dev(r, y, xct)
                )

            if offs[NZ - 1 - i] == 0:
                pl.when(xct != xc)(go)
            else:
                go()

    chunk = pl.ds(pl.multiple_of(zl * CW + kme * PC, PC), PC)

    def relay_back(part):
        @pl.when(active)
        def _():
            got, put = zr[part], f1[part]
            got[mine] = sz[NZ - 1, span(part), cols(kme)]
            wait(got.at[pl.ds(0, NZ * NXC - 1)], zr_recv.at[part])
            for s in range(NS):
                j = src_ref[s]
                put[s] = (got[j].astype(F32) + got[j + NS].astype(F32)).astype(BF16)
            fin[span(part), chunk] = put[me_e]

            for n in range(ZL):
                s_z = rem(zl + n, ZL)
                z = ZL * half(p, s_z) + s_z
                for q in range(NXC):
                    if n or q:
                        remote(
                            put.at[s_z * NXC + xcs[q]], fin.at[span(part), chunk], f_send.at[part], f_recv.at[part],
                            dev(z, y, xcs[q]),
                        )

    compute(0)
    for v in range(units + BACK_LAG + LAST_LAG):
        if v < units:
            send_parts(v)
        passing = v - BACK_LAG
        if 0 <= passing < units:
            add_passing(passing)
        if v + 1 < NZ:
            compute(v + 1)
        if 0 <= passing < units:
            send_passing(passing)
        done = v - BACK_LAG - LAST_LAG
        if done >= 0:
            add_own(done)
            if done == 2:
                stats_next(3)
            if done == 3:
                stats_send(3)
            if done == NZ + 1:
                stats_out(stats_sum(3))
            send_relays(done)
            if done == NZ + 3:
                relay_back(1)
    relay_back(0)

    def returned(part):
        @pl.when(active)
        def _():
            wait(send2[part].at[pl.ds(0, ZL * KP - 1)], f_recv.at[part])

        @pl.when(jnp.logical_not(active))
        def _():
            wait(send2[part].at[pl.ds(0, ZL * KP)], f_recv.at[part])

    returned(1)
    returned(0)
    copy_out = pltpu.make_async_copy(fin, out_hbm, in_sem)
    copy_out.start()

    @pl.when(active)
    def _():
        wait(send1.at[pl.ds(0, ZL - 1)], s1_send)
        if KP > 1:
            wait(send1.at[0, :, pl.ds(0, CW - PC)], s1_send)
        for part in range(2):
            wait(zr[part].at[pl.ds(0, NZ * NXC - 1)], s2_send.at[part])
            wait(zr[part].at[pl.ds(0, NZ * KP - 1)], z_send.at[part])
            wait(zr[part].at[pl.ds(0, NS - 1)], f_send.at[part])

    @pl.when(jnp.logical_not(active))
    def _():
        wait(send1, s1_send)
        for part in range(2):
            wait(zr[part].at[pl.ds(0, NZ * KP)], z_send.at[part])

    wait(pbuf.at[pl.ds(0, 3 * NZ // Y)], y_send)
    wait(pbuf.at[pl.ds(0, 3 * NZ // Y)], r_send)
    pltpu.make_async_copy(st_out, stats_hbm, st_sem).wait()
    copy_out.wait()


def on_device(L, tokens, routed, expert_ids, norm_gain, gate_weight, up_weight, down_weight, old_place, new_place, probe_ids):
    NZ, NXC, Y, ZL, KP, NS, CW, rows = L.NZ, L.NXC, L.Y, L.ZL, L.KP, L.NS, L.CW, L.ROWS
    smem = pl.BlockSpec(memory_space=pltpu.SMEM)
    vmem = pl.BlockSpec(memory_space=pltpu.VMEM)
    anyspace = pl.BlockSpec(memory_space=pl.ANY)
    dma = pltpu.SemaphoreType.DMA
    V = pltpu.VMEM

    def pieces(n):
        return [V((n, size, PC), BF16) for _, size in L.PARTS]

    scratch = [
        V((L.TOKS, L.D), BF16), V((L.D // 128, 128), F32),
        V((ZL, CW, L.HID), BF16), V((ZL, CW, L.HID), BF16), V((ZL, L.HID, CW), BF16),
        V((ZL, rows, CW), BF16), *pieces(NS), *pieces(NS),
        V((NZ, Y, rows, CW), BF16),
        V((L.ZH, Y * rows, L.HID), F32), V((L.ZH, Y * rows, L.HID), F32), V((L.ZH, Y * rows, L.HID), BF16),
        V((NZ, Y, rows, CW), BF16), V((NZ, rows, CW), BF16), V((NZ, 2, rows, CW), BF16),
        V((NZ, rows, CW), BF16), V((NZ, rows, CW), BF16),
        *pieces(NZ * NXC), *pieces(NS), V((rows, L.D), BF16),
        V((Y, 8, 128), F32), V((NZ, 8, 128), F32), V((L.X, 8, 128), F32), V((L.C, 8, 128), F32), V((8, 128), F32),
        pltpu.SMEM((NS,), jnp.int32), pltpu.SMEM((NS,), jnp.int32),
        dma, dma, dma, dma((2,)), dma((2,)), dma((2 * NZ,)), dma, dma((2 * NZ,)), dma((2 * NZ,)), dma((2 * NZ,)),
        dma, dma((2 * NZ,)), dma((2 * NZ,)), dma((2 * NZ,)), dma((2,)), dma((2,)), dma((2,)), dma((2,)), dma((4,)), dma((4,)), dma,
    ]
    stats, probe_out = pl.pallas_call(
        functools.partial(kernel, L, tokens),
        out_shape=(
            jax.ShapeDtypeStruct((8, 128), F32),
            jax.ShapeDtypeStruct((rows, L.D), BF16),
        ),
        in_specs=[smem, smem, smem, vmem, vmem, anyspace, anyspace, anyspace, anyspace],
        out_specs=(anyspace, anyspace),
        scratch_shapes=scratch,
        compiler_params=pltpu.CompilerParams(
            collective_id=0, has_side_effects=True, vmem_limit_bytes=60 * 1024 * 1024
        ),
        name="probe_pass",
    )(
        old_place, new_place, probe_ids, expert_ids.T, norm_gain.reshape(L.D // 128, 128),
        routed, gate_weight[0], up_weight[0], down_weight[0],
    )
    counts, energy = stats[0, :EXP_DEV], stats[1, :EXP_DEV]
    return counts * (EXP_DEV * NS) / (tokens * TOP), energy / counts, probe_out


def build(mesh, L, tokens):
    both = ("dp", "expert")
    return jax.shard_map(
        functools.partial(on_device, L, tokens),
        mesh=mesh,
        in_specs=(
            P(both, None), P(both, None), P(), P("expert", None, "dp"), P("expert", None, "dp"),
            P("expert", "dp", None), P(), P(), P(both),
        ),
        out_specs=(P("expert"), P("expert"), P(both, None)),
        check_vma=False,
    )


def solution(mesh):
    L = Layout()
    return build(mesh, L, L.TOKS * L.ZH * L.Y * L.NS)
```

```python
import functools

import jax
import jax.numpy as jnp
from jax import lax
from jax.experimental import pallas as pl
from jax.experimental.pallas import tpu as pltpu
from jax.sharding import PartitionSpec as P

MESH = pl.DeviceIdType.MESH
F32 = jnp.float32
BF16 = jnp.bfloat16
EXP_DEV = 8
TOP = 8
EPS = 1e-06
PC = 256
LAG = 2
BACK_LAG = 3
LAST_LAG = 2


class Layout:
    def __init__(self, zh=2, y=4, zl=4, x=4, c=2, pieces=7, rows=40, toks=128, hid=256):
        self.ZH, self.Y, self.ZL, self.X, self.C = zh, y, zl, x, c
        self.KP, self.ROWS, self.TOKS, self.HID = pieces, rows, toks, hid
        self.NZ, self.NXC = zh * zl, x * c
        self.NS = zl * x * c
        self.CW = pieces * PC
        self.D = zl * self.CW
        head = rows * 2 // 5 // 8 * 8 or rows // 2
        self.PARTS = ((0, head), (head, rows - head))


def kernel(
    L, tokens,
    old_ref, new_ref, pid_ref, ids_ref, gain_ref, routed_hbm, gate_hbm, up_hbm, down_hbm,
    stats_hbm, out_hbm,
    routed_v, gain_v, gate_v, up_v, down_v,
    send1, recv1_a, recv1_b, send2_a, send2_b, xbuf, gacc, uacc, hid,
    pbuf, ra, rb, bs, sz, zr_a, zr_b, f1_a, f1_b, fin,
    st_y, st_z, st_x, st_c, st_out, tgt_ref, src_ref,
    in_sem, w_sem, s1_send, s1_recv, s2_send, s2_recv, y_send, y_recv, yf_recv,
    r_send, ra_recv, rb0_recv, rb1_recv, z_send, zr_recv, f_send, f_recv, st_send, st_recv, st_sem, out_sem,
):
    Y, ZL, X, C, KP, NZ, NXC, NS, CW = L.Y, L.ZL, L.X, L.C, L.KP, L.NZ, L.NXC, L.NS, L.CW
    rows = L.ROWS
    PARTS = L.PARTS
    recv1, send2, zr, f1 = (recv1_a, recv1_b), (send2_a, send2_b), (zr_a, zr_b), (f1_a, f1_b)
    me_d, me_e = lax.axis_index("dp"), lax.axis_index("expert")
    div, rem = lax.div, lax.rem
    zh, y = div(me_d, Y), rem(me_d, Y)
    zl, xc = div(me_e, NXC), rem(me_e, NXC)
    x, c = div(xc, C), rem(xc, C)
    p = zh * ZL + zl
    kme = rem(xc - C * zl + C * NXC, NXC)
    active = kme < KP
    mine = p * NXC + xc
    offs = [((t + 1) // 2) * (2 * (t % 2) - 1) for t in range(NZ)]
    REACH = ZL // 2
    zs = [rem(p + o + NZ, NZ) for o in offs]
    xcs = [rem(xc + q, NXC) for q in range(NXC)]

    def dev(z, yy, xcc):
        return (div(z, ZL) * Y + yy, rem(z, ZL) * NXC + xcc)

    def half(r, z_low):
        return div(rem(r - z_low + ZL // 2 - 1 + rem(r, 2) + NZ, NZ), ZL)

    def span(part):
        return pl.ds(*PARTS[part])

    def cols(k):
        return pl.ds(pl.multiple_of(k * PC, PC), PC)

    def remote(src, dst, send, recv, where):
        pltpu.make_async_remote_copy(
            src_ref=src, dst_ref=dst, send_sem=send, recv_sem=recv, device_id=where, device_id_type=MESH
        ).start()

    def wait(ref, sem):
        pltpu.make_async_copy(ref, ref, sem).wait()

    copy_in = pltpu.make_async_copy(routed_hbm, routed_v, in_sem)
    copy_in.start()
    barrier = pltpu.get_barrier_semaphore()

    for t in reversed(range(NZ)):
        for q in reversed(range(NXC)):
            if (t or q) and abs(offs[t]) <= REACH:
                pl.semaphore_signal(barrier, inc=1, device_id=dev(zs[t], y, xcs[q]), device_id_type=MESH)
    for dy in range(1, Y):
        pl.semaphore_signal(barrier, inc=1, device_id=dev(p, rem(y + dy, Y), xc), device_id_type=MESH)

    gain_v[...] = gain_ref[...].astype(F32)
    lane = lax.broadcasted_iota(jnp.int32, (8, L.TOKS), 1)
    sub = lax.broadcasted_iota(jnp.int32, (8, L.TOKS), 0)
    picks = []
    for b in range(rows // 8):
        want = jnp.zeros((8, L.TOKS), jnp.int32)
        for i in range(8):
            want = jnp.where(sub == i, pid_ref[b * 8 + i], want)
        picks.append((lane == want).astype(F32))
    select = jnp.concatenate(picks, axis=0).astype(BF16)

    copy_in.wait()
    for hbm, v in ((gate_hbm, gate_v), (up_hbm, up_v)):
        for m in range(ZL):
            pltpu.make_async_copy(hbm.at[pl.ds(m * CW, CW), :], v.at[m], w_sem).start()
    for m in range(ZL):
        pltpu.make_async_copy(down_hbm.at[:, pl.ds(m * CW, CW)], down_v.at[m], w_sem).start()

    square = jnp.zeros((rows, 1), F32)
    for m in range(ZL):
        picked = jnp.dot(select, routed_v[:, m * CW : (m + 1) * CW], preferred_element_type=F32)
        square += jnp.sum(picked * picked, axis=1, keepdims=True)
        send1[m] = picked.astype(BF16)
    scale = lax.rsqrt(square / L.D + EPS)
    for m in range(ZL):
        for t in range(CW // 128):
            tile = m * (CW // 128) + t
            v = send1[m, :, t * 128 : (t + 1) * 128].astype(F32)
            send1[m, :, t * 128 : (t + 1) * 128] = (v * scale * gain_v[tile : tile + 1, :]).astype(BF16)

    pl.semaphore_wait(barrier, sum(abs(o) <= REACH for o in offs) * NXC - 1 + Y - 1)

    near = [(m, m + ZL * rem(half(m, zl) + zh, 2)) for m in range(ZL)]
    def to_relays(part):
        for n in range(KP):
            k = rem(xc + n, KP)
            for m, r in near:
                xct = rem(k + C * m, NXC)

                @pl.when(r * NXC + xct != mine)
                def _():
                    remote(
                        send1.at[m, span(part), cols(k)], recv1[part].at[me_e], s1_send, s1_recv.at[part],
                        dev(r, y, xct),
                    )

    to_relays(0)

    def find(out, values, among):
        @pl.loop(0, NS)
        def _(i):
            value = values[i]
            found = 0
            for j in range(NS):
                found = jnp.where(among[j] == value, j, found)
            out[i] = found

    find(tgt_ref, old_ref, new_ref)
    find(src_ref, new_ref, old_ref)

    def squares(i, acc):
        v = routed_v[:, pl.ds(pl.multiple_of(i * PC, PC), PC)].astype(F32)
        return acc + v * v

    total = lax.fori_loop(0, L.D // PC, squares, jnp.zeros((L.TOKS, PC), F32))
    mean_square = jnp.sum(total, axis=1, keepdims=True) / L.D
    ids = ids_ref[...].astype(F32).T
    expert = lax.broadcasted_iota(jnp.int32, (L.TOKS, 256), 1).astype(F32)
    onehot = jnp.zeros((L.TOKS, 256), F32)
    for k in range(TOP):
        onehot += (ids[:, k : k + 1] == expert).astype(F32)
    counts = jnp.sum(onehot, axis=0, keepdims=True)
    energy = jnp.sum(onehot * mean_square, axis=0, keepdims=True)
    stats = jnp.concatenate(
        [counts[:, :128], counts[:, 128:], energy[:, :128], energy[:, 128:], jnp.zeros((4, 128), F32)], axis=0
    )
    rounds = (
        (st_y, Y, y, lambda o: dev(p, o, xc)),
        (st_z, NZ, p, lambda o: dev(o, y, xc)),
        (st_x, X, x, lambda o: dev(p, y, o * C + c)),
        (st_c, C, c, lambda o: dev(p, y, x * C + o)),
    )

    def stats_store(n, value):
        buf, _, own, _ = rounds[n]
        buf[own] = value

    def stats_send(n):
        buf, size, own, where = rounds[n]
        for step in range(1, size):
            remote(buf.at[own], buf.at[own], st_send.at[n], st_recv.at[n], where(rem(own + step, size)))

    def stats_sum(n):
        buf, size, own, _ = rounds[n]
        if size > 1:
            wait(buf.at[pl.ds(0, size - 1)], st_recv.at[n])
            wait(buf.at[pl.ds(0, size - 1)], st_send.at[n])
        value = buf[0]
        for o in range(1, size):
            value += buf[o]
        return value

    def stats_out(value):
        where = lax.broadcasted_iota(jnp.int32, (2, 128), 0) * 128 + lax.broadcasted_iota(jnp.int32, (2, 128), 1)
        row, col = lax.broadcasted_iota(jnp.int32, (8, 128), 0), lax.broadcasted_iota(jnp.int32, (8, 128), 1)
        tile = jnp.zeros((8, 128), F32)
        for i in range(EXP_DEV):
            hit = where == me_e * EXP_DEV + i
            for n in range(2):
                one = jnp.sum(jnp.where(hit, value[2 * n : 2 * n + 2], 0.0))
                tile = jnp.where((row == n) & (col == i), one, tile)
        st_out[...] = tile
        pltpu.make_async_copy(st_out, stats_hbm, st_sem).start()

    def stats_next(n):
        stats_store(n, stats_sum(n - 1))

    stats_store(0, stats)
    to_relays(1)

    def relay(part):
        @pl.when(active)
        def _():
            got, put = recv1[part], send2[part]
            got[me_e] = send1[zl, span(part), cols(kme)]
            wait(got.at[pl.ds(0, NS - 1)], s1_recv.at[part])
            for j in range(NS):
                put[j] = got[tgt_ref[j]]
            xbuf[p, y, span(part), cols(kme)] = got[tgt_ref[me_e]]

    def to_holders(part, ts):
        @pl.when(active)
        def _():
            for t in ts:
                for q in range(NXC):
                    if t or q:
                        remote(
                            send2[part].at[rem(zs[t], ZL) * NXC + xcs[q]],
                            xbuf.at[p, y, span(part), cols(kme)],
                            s2_send.at[part],
                            s2_recv.at[part * NZ + p],
                            dev(zs[t], y, xcs[q]),
                        )

    slot = tgt_ref[me_e]
    slot_z = div(slot, NXC)
    ynext, yprev, yopp = rem(y + 1, Y), rem(y + Y - 1, Y), rem(y + 2, Y)

    pairs = []
    for a in range(NZ):
        for b in range(a + 1, NZ):
            if (offs[a] - offs[b]) % NZ == ZL:
                pairs.append((b, a))
    pairs.sort()
    orders = (list(range(NZ)), list(range(NZ)))

    def place(u):
        return u // NZ, orders[u // NZ][u % NZ]

    def ring(i):
        return zs[i]

    def block(u, who):
        part, i = place(u)
        return xbuf.at[ring(i), who, span(part)]

    units = 2 * NZ

    def own_group(u):
        part, i = place(u)
        mine_here = block(u, y)
        sem = s2_recv.at[part * NZ + ring(i)]
        if offs[i] == 0:
            @pl.when(active)
            def _():
                if KP > 1:
                    wait(xbuf.at[p, y, span(part), pl.ds(0, CW - PC)], sem)

            @pl.when(jnp.logical_not(active))
            def _():
                wait(mine_here, sem)
        else:
            wait(mine_here, sem)
        remote(mine_here, mine_here, y_send, y_recv.at[u], dev(p, ynext, xc))
        remote(mine_here, mine_here, y_send, y_recv.at[units + u], dev(p, yprev, xc))

    def forward(u):
        way = rem(c + u, 2)
        came = rem(y + Y - 1 + 2 * way, Y)
        wait(block(u, came), y_recv.at[way * units + u])
        remote(block(u, came), block(u, came), y_send, yf_recv.at[u], dev(p, rem(came + 2, Y), xc))

    def arrived(u):
        way = 1 - rem(c + u, 2)
        wait(block(u, rem(y + Y - 1 + 2 * way, Y)), y_recv.at[way * units + u])
        wait(block(u, yopp), yf_recv.at[u])

    first = [True]

    def project(a, b):
        for i in (a, b):
            arrived(i)
            arrived(NZ + orders[1].index(i))
        m = rem(ring(a), ZL)
        near = half(m, slot_z) == 0
        lhs = jnp.concatenate([xbuf[m].reshape(Y * rows, CW), xbuf[m + ZL].reshape(Y * rows, CW)], axis=0)
        opening = first[0]
        first[0] = False
        if opening:
            wait(gate_v, w_sem)
            wait(up_v, w_sem)
            wait(down_v, w_sem)
        for weight, acc in ((gate_v, gacc), (up_v, uacc)):
            value = jnp.dot(lhs, weight[m], preferred_element_type=F32)
            a, b = value[: Y * rows], value[Y * rows :]
            for h, part in ((0, jnp.where(near, a, b)), (1, jnp.where(near, b, a))):
                if opening:
                    acc[h] = part
                else:
                    acc[h] += part

    relay(0)
    to_holders(0, range(NZ))
    stats_send(0)
    own_group(0)
    relay(1)
    to_holders(1, orders[1][: NZ // 2])
    for u in range(1, units):
        own_group(u)
        if u - 1 in range(NZ // 2):
            to_holders(1, orders[1][NZ // 2 + u - 1 : NZ // 2 + u])
        if u >= LAG:
            forward(u - LAG)
        if u == units // 4:
            stats_next(1)
        if u == units // 4 + 1:
            stats_send(1)
        if u == units - 3:
            stats_next(2)
        if u == units - 2:
            stats_send(2)
    for u in range(units - LAG, units):
        forward(u)
        if u < units - 1 and len(pairs) > 2:
            project(*pairs.pop(0)[::-1])
    for b, a in pairs:
        project(a, b)

    g = gacc[...]
    hid[...] = (g / (1.0 + jnp.exp(-g)) * uacc[...]).astype(BF16)

    def back(i):
        return ring(NZ - 1 - i)

    def sign(v):
        to = rem(y + 1 + 2 * rem(c + v, 2), Y)
        return to, rem(to + 2, Y)

    def compute(i):
        r = back(i)
        value = jnp.dot(hid[half(r, slot_z)], down_v[rem(r, ZL)], preferred_element_type=F32)
        pbuf[i] = value.astype(BF16).reshape(Y, rows, CW)

    def unit(v):
        return 1 - v // NZ, v % NZ

    def send_parts(v):
        part, i = unit(v)
        to, _ = sign(v)
        remote(pbuf.at[i, yopp, span(part)], ra.at[i, span(part)], r_send, ra_recv.at[v], dev(p, to, xc))

    def add_passing(v):
        part, i = unit(v)
        to, _ = sign(v)
        wait(ra.at[i, span(part)], ra_recv.at[v])
        bs[i, span(part)] = (pbuf[i, to, span(part)].astype(F32) + ra[i, span(part)].astype(F32)).astype(BF16)

    def send_passing(v):
        part, i = unit(v)
        to, other = sign(v)
        remote(bs.at[i, span(part)], rb.at[i, 1, span(part)], r_send, rb1_recv.at[v], dev(p, to, xc))
        remote(pbuf.at[i, other, span(part)], rb.at[i, 0, span(part)], r_send, rb0_recv.at[v], dev(p, other, xc))

    def add_own(v):
        part, i = unit(v)
        rw = span(part)
        wait(rb.at[i, 0, rw], rb0_recv.at[v])
        wait(rb.at[i, 1, rw], rb1_recv.at[v])
        sz[i, rw] = (pbuf[i, y, rw].astype(F32) + rb[i, 0, rw].astype(F32) + rb[i, 1, rw].astype(F32)).astype(BF16)

    def send_relays(v):
        part, i = unit(v)
        r = back(i)
        m = rem(r, ZL)
        for n in range(KP):
            k = rem(xc + n, KP)
            xct = rem(k + C * m, NXC)

            def go():
                remote(
                    sz.at[i, span(part), cols(k)], zr[part].at[mine], z_send.at[part], zr_recv.at[part], dev(r, y, xct)
                )

            if offs[NZ - 1 - i] == 0:
                pl.when(xct != xc)(go)
            else:
                go()

    chunk = pl.ds(pl.multiple_of(zl * CW + kme * PC, PC), PC)

    def relay_back(part):
        @pl.when(active)
        def _():
            got, put = zr[part], f1[part]
            got[mine] = sz[NZ - 1, span(part), cols(kme)]
            wait(got.at[pl.ds(0, NZ * NXC - 1)], zr_recv.at[part])
            for s in range(NS):
                j = src_ref[s]
                put[s] = (got[j].astype(F32) + got[j + NS].astype(F32)).astype(BF16)
            fin[span(part), chunk] = put[me_e]

            for n in range(ZL):
                s_z = rem(zl + n, ZL)
                z = ZL * half(p, s_z) + s_z
                for q in range(NXC):
                    if n or q:
                        remote(
                            put.at[s_z * NXC + xcs[q]], fin.at[span(part), chunk], f_send.at[part], f_recv.at[part],
                            dev(z, y, xcs[q]),
                        )

    compute(0)
    for v in range(units + BACK_LAG + LAST_LAG):
        if v < units:
            send_parts(v)
        passing = v - BACK_LAG
        if 0 <= passing < units:
            add_passing(passing)
        if v + 1 < NZ:
            compute(v + 1)
        if 0 <= passing < units:
            send_passing(passing)
        done = v - BACK_LAG - LAST_LAG
        if done >= 0:
            add_own(done)
            if done == 2:
                stats_next(3)
            if done == 3:
                stats_send(3)
            if done == NZ + 1:
                stats_out(stats_sum(3))
            send_relays(done)
            if done == NZ + 3:
                relay_back(1)
    relay_back(0)

    def returned(part):
        @pl.when(active)
        def _():
            wait(send2[part].at[pl.ds(0, ZL * KP - 1)], f_recv.at[part])

        @pl.when(jnp.logical_not(active))
        def _():
            wait(send2[part].at[pl.ds(0, ZL * KP)], f_recv.at[part])

    def leave(part):
        return pltpu.make_async_copy(fin.at[span(part)], out_hbm.at[span(part)], out_sem.at[part])

    returned(1)
    leave(1).start()
    returned(0)
    leave(0).start()

    @pl.when(active)
    def _():
        wait(send1.at[pl.ds(0, ZL - 1)], s1_send)
        if KP > 1:
            wait(send1.at[0, :, pl.ds(0, CW - PC)], s1_send)
        for part in range(2):
            wait(zr[part].at[pl.ds(0, NZ * NXC - 1)], s2_send.at[part])
            wait(zr[part].at[pl.ds(0, NZ * KP - 1)], z_send.at[part])
            wait(zr[part].at[pl.ds(0, NS - 1)], f_send.at[part])

    @pl.when(jnp.logical_not(active))
    def _():
        wait(send1, s1_send)
        for part in range(2):
            wait(zr[part].at[pl.ds(0, NZ * KP)], z_send.at[part])

    wait(pbuf.at[pl.ds(0, 3 * NZ // Y)], y_send)
    wait(pbuf.at[pl.ds(0, 3 * NZ // Y)], r_send)
    pltpu.make_async_copy(st_out, stats_hbm, st_sem).wait()
    for part in range(2):
        leave(part).wait()


def on_device(L, tokens, routed, expert_ids, norm_gain, gate_weight, up_weight, down_weight, old_place, new_place, probe_ids):
    NZ, NXC, Y, ZL, KP, NS, CW, rows = L.NZ, L.NXC, L.Y, L.ZL, L.KP, L.NS, L.CW, L.ROWS
    smem = pl.BlockSpec(memory_space=pltpu.SMEM)
    vmem = pl.BlockSpec(memory_space=pltpu.VMEM)
    anyspace = pl.BlockSpec(memory_space=pl.ANY)
    dma = pltpu.SemaphoreType.DMA
    V = pltpu.VMEM

    def pieces(n):
        return [V((n, size, PC), BF16) for _, size in L.PARTS]

    scratch = [
        V((L.TOKS, L.D), BF16), V((L.D // 128, 128), F32),
        V((ZL, CW, L.HID), BF16), V((ZL, CW, L.HID), BF16), V((ZL, L.HID, CW), BF16),
        V((ZL, rows, CW), BF16), *pieces(NS), *pieces(NS),
        V((NZ, Y, rows, CW), BF16),
        V((L.ZH, Y * rows, L.HID), F32), V((L.ZH, Y * rows, L.HID), F32), V((L.ZH, Y * rows, L.HID), BF16),
        V((NZ, Y, rows, CW), BF16), V((NZ, rows, CW), BF16), V((NZ, 2, rows, CW), BF16),
        V((NZ, rows, CW), BF16), V((NZ, rows, CW), BF16),
        *pieces(NZ * NXC), *pieces(NS), V((rows, L.D), BF16),
        V((Y, 8, 128), F32), V((NZ, 8, 128), F32), V((L.X, 8, 128), F32), V((L.C, 8, 128), F32), V((8, 128), F32),
        pltpu.SMEM((NS,), jnp.int32), pltpu.SMEM((NS,), jnp.int32),
        dma, dma, dma, dma((2,)), dma((2,)), dma((2 * NZ,)), dma, dma((4 * NZ,)), dma((2 * NZ,)),
        dma, dma((2 * NZ,)), dma((2 * NZ,)), dma((2 * NZ,)), dma((2,)), dma((2,)), dma((2,)), dma((2,)), dma((4,)), dma((4,)), dma, dma((2,)),
    ]
    stats, probe_out = pl.pallas_call(
        functools.partial(kernel, L, tokens),
        out_shape=(
            jax.ShapeDtypeStruct((8, 128), F32),
            jax.ShapeDtypeStruct((rows, L.D), BF16),
        ),
        in_specs=[smem, smem, smem, vmem, vmem, anyspace, anyspace, anyspace, anyspace],
        out_specs=(anyspace, anyspace),
        scratch_shapes=scratch,
        compiler_params=pltpu.CompilerParams(
            collective_id=0, has_side_effects=True, vmem_limit_bytes=60 * 1024 * 1024
        ),
        name="probe_pass",
    )(
        old_place, new_place, probe_ids, expert_ids.T, norm_gain.reshape(L.D // 128, 128),
        routed, gate_weight[0], up_weight[0], down_weight[0],
    )
    counts, energy = stats[0, :EXP_DEV], stats[1, :EXP_DEV]
    return counts * (EXP_DEV * NS) / (tokens * TOP), energy / counts, probe_out


def build(mesh, L, tokens):
    both = ("dp", "expert")
    return jax.shard_map(
        functools.partial(on_device, L, tokens),
        mesh=mesh,
        in_specs=(
            P(both, None), P(both, None), P(), P("expert", None, "dp"), P("expert", None, "dp"),
            P("expert", "dp", None), P(), P(), P(both),
        ),
        out_specs=(P("expert"), P("expert"), P(both, None)),
        check_vma=False,
    )


def solution(mesh):
    L = Layout()
    return build(mesh, L, L.TOKS * L.ZH * L.Y * L.NS)
```
